32 devices in a mesh: fsdp: 8 (over z, core), cols: 4 (over y, x).
Axes of the slice: x: 2, y: 2, z: 4, core: 2. Of those that a mesh axis runs over, the one named last changes fastest.
Arguments:
- one_query: float32 [4096, 4096], P('fsdp', 'cols'), may hold values from -0.125 to 0.125
- other_query: float32 [4096, 4096], P('fsdp', 'cols'), may hold values from -0.09375 to 0.09375
- one_key: float32 [4096, 4096], P('fsdp', 'cols'), may hold values from -0.125 to 0.125
- other_key: float32 [4096, 4096], P('fsdp', 'cols'), may hold values from -0.09375 to 0.09375
- one_value: float32 [4096, 4096], P('fsdp', 'cols'), may hold values from -0.125 to 0.125
- other_value: float32 [4096, 4096], P('fsdp', 'cols'), may hold values from -0.09375 to 0.09375
- mix_share: float32 [4096], P('fsdp'), may hold values from 0.2 to 0.8
- norm_train: float32 [4096], P(('fsdp', 'cols')), may hold values from 0.25 to 1.75
- norm_step: float32 [4096], P(('fsdp', 'cols')), may hold values from -0.3 to 0.3
Outputs:
- final_query: bfloat16 [4096, 4096], P(None, 'cols')
- final_key: bfloat16 [4096, 4096], P(None, 'cols')
- final_value: bfloat16 [4096, 4096], P(None, 'cols')
- scale_query: float32 [4096], P('cols')
- scale_key: float32 [4096], P('cols')
- scale_value: float32 [4096], P('cols')
- serve_norm: bfloat16 [4096], replicated
The draws below stay inside these ranges and needn't reach their ends.
All inputs are finite; a program needn't handle non-finite values.
Results may differ from the reference program's by a relative error of at most 0.0004.
Values may be sent and summed in bfloat16 or wider, within the bound.
A program may use at most 128 MiB of HBM per device.

```python
import jax
import jax.numpy as jnp
from jax import lax

D_MODEL = 4096
Q_DIM = 4096
KV_DIM = 4096


def with_spikes(values, stream_key, source, target, shards_of, factor):
    owner, partner = [(jnp.arange(values.shape[position]) // (values.shape[position] // shards_of)).reshape([-1 if axis == position else 1 for axis in range(values.ndim)]) for position in (source, target)]
    chosen = jax.random.permutation(stream_key, shards_of)[partner]
    strong = (owner == chosen) | (owner == (partner + shards_of // 2) % shards_of)
    return jnp.where(strong, factor * values, values)


def level_of(rng, extent, split, low, top_value):
    loudness = 1.0
    for position, parts in split:
        steps = jax.random.uniform(jax.random.fold_in(jax.random.fold_in(rng, 6), position), (parts,), jnp.float32, low / len(split), top_value / len(split))
        loudness = loudness * jnp.repeat(jnp.exp(steps), extent[position] // parts).reshape((-1,) + (1,) * (len(extent) - 1 - position))
    return loudness


def noise(stream_key, dims, deviation, limit, shards=(), held_as=jnp.bfloat16):
    factor_of = level_of(stream_key, dims, shards, -0.22, 0.18) if shards else 1.0
    drawn = jax.random.normal(stream_key, dims, jnp.float32) * deviation * factor_of
    return jnp.minimum(jnp.maximum(drawn, -limit), limit).astype(held_as)


def gaussian_with(stream_key, dims, scale, most, cuts, heavy, dtype=jnp.bfloat16):
    values = scale * jax.random.normal(stream_key, dims, jnp.float32)
    if cuts:
        values = values * level_of(stream_key, dims, cuts, -0.22, 0.18)
    return jnp.clip(with_spikes(values, jax.random.fold_in(stream_key, 3), *heavy), -most, most).astype(dtype)


def setup_inputs(seed: int = 0) -> dict:
    key_list = jax.random.split(jax.random.key(seed), 10)
    one_query = gaussian_with(key_list[0], (D_MODEL, Q_DIM), D_MODEL ** -0.5, 0.125, ((0, 8), (1, 4)), (0, 1, 8, 2.0), jnp.float32)
    other_query = noise(key_list[1], (D_MODEL, Q_DIM), D_MODEL ** -0.5, 0.09375, ((0, 8), (1, 4)), jnp.float32)
    one_key = gaussian_with(key_list[2], (D_MODEL, KV_DIM), D_MODEL ** -0.5, 0.125, ((0, 8), (1, 4)), (0, 1, 8, 2.0), jnp.float32)
    other_key = noise(key_list[3], (D_MODEL, KV_DIM), D_MODEL ** -0.5, 0.09375, ((0, 8), (1, 4)), jnp.float32)
    one_value = gaussian_with(key_list[4], (D_MODEL, KV_DIM), D_MODEL ** -0.5, 0.125, ((0, 8), (1, 4)), (0, 1, 8, 2.0), jnp.float32)
    other_value = noise(key_list[5], (D_MODEL, KV_DIM), D_MODEL ** -0.5, 0.09375, ((0, 8), (1, 4)), jnp.float32)
    mix_share = jnp.clip(0.2 + 0.6 * jax.random.uniform(key_list[6], (D_MODEL,), jnp.float32) ** level_of(key_list[6], (D_MODEL,), ((0, 8),), -0.2, 0.2), 0.2, 0.8)
    norm_train = jnp.clip(1.0 + 0.15 * jax.random.normal(key_list[7], (D_MODEL,), jnp.float32), 0.25, 1.75)
    norm_step = jnp.clip(jax.random.uniform(key_list[8], (D_MODEL,), jnp.float32, -0.3, 0.3) * level_of(key_list[8], (D_MODEL,), ((0, 32),), -0.4, 0.0), -0.3, 0.3)
    return dict(one_query=one_query, other_query=other_query, one_key=one_key, other_key=other_key, one_value=one_value, other_value=other_value, mix_share=mix_share, norm_train=norm_train, norm_step=norm_step)


def reference(one_query, other_query, one_key, other_key, one_value, other_value, mix_share, norm_train, norm_step):
    result_query = mix_share[:, None] * one_query + (1.0 - mix_share[:, None]) * other_query
    result_key = mix_share[:, None] * one_key + (1.0 - mix_share[:, None]) * other_key
    result_value = mix_share[:, None] * one_value + (1.0 - mix_share[:, None]) * other_value
    scale_query = jnp.sqrt(lax.optimization_barrier(jnp.sum(result_query * result_query, axis=0)))
    final_query = (result_query / scale_query).astype(jnp.bfloat16)
    scale_key = jnp.sqrt(lax.optimization_barrier(jnp.sum(result_key * result_key, axis=0)))
    final_key = (result_key / scale_key).astype(jnp.bfloat16)
    scale_value = jnp.sqrt(lax.optimization_barrier(jnp.sum(result_value * result_value, axis=0)))
    final_value = (result_value / scale_value).astype(jnp.bfloat16)
    serve_norm = (norm_train + norm_step).astype(jnp.bfloat16)
    return (final_query, final_key, final_value, scale_query, scale_key, scale_value, serve_norm)
```

```python
import functools

import jax
import jax.numpy as jnp
from jax import lax
from jax.experimental import pallas as pl
from jax.experimental.pallas import tpu as pltpu
from jax.sharding import PartitionSpec as P

MESH = pl.DeviceIdType.MESH
LANES = 128
CHUNKS = 4


def gather_kernel(F, C, *refs):
    ins, mix_ref, train_ref, step_ref = refs[0:6], refs[6], refs[7], refs[8]
    outs, scale_out, norm_out = refs[9:12], refs[12], refs[13]
    (held, mixb, sums, in_sem, sum_send, sum_recv, norm_send1, norm_recv1,
     norm_send2, norm_recv2, up_send, down_send, pair_send, line_recv, pair_recv) = refs[14:]
    rows, width = ins[0].shape
    Z = F // 2
    me = lax.axis_index("fsdp")
    col = lax.axis_index("cols")
    z = me // 2
    core = lax.rem(me, 2)
    part = rows // CHUNKS
    K = 3 * CHUNKS

    def at(f):
        return {"fsdp": f}

    loads = [pltpu.make_async_copy(ins[i], held.at[i], in_sem.at[i]) for i in range(6)]
    for load in loads:
        load.start()

    barrier = pltpu.get_barrier_semaphore()
    for d in range(1, F):
        pl.semaphore_signal(barrier, inc=1, device_id=(lax.rem(me + d, F), col), device_id_type=MESH)
    for d in range(1, C):
        pl.semaphore_signal(barrier, inc=1, device_id=(me, lax.rem(col + d, C)), device_id_type=MESH)

    for g in range(rows // LANES):
        row = mix_ref[pl.ds(g, 1), :]
        mixb[pl.ds(g * LANES, LANES), :] = jnp.broadcast_to(row, (LANES, LANES)).T
    norm_out[me, col] = train_ref[...] + step_ref[...]

    def mix(a):
        loads[2 * a].wait()
        loads[2 * a + 1].wait()

        def body(i, acc):
            r = pl.ds(pl.multiple_of(i * 8, 8), 8)
            m = mixb[r, :]
            n = 1.0 - m
            new = []
            for j in range(width // LANES):
                c = pl.ds(j * LANES, LANES)
                v = m * held[2 * a, r, c] + n * held[2 * a + 1, r, c]
                held[2 * a, r, c] = v
                new.append(acc[j] + v * v)
            return tuple(new)

        zero = jnp.zeros((8, LANES), jnp.float32)
        acc = lax.fori_loop(0, rows // 8, body, (zero,) * (width // LANES), unroll=2)
        for j in range(width // LANES):
            sums[a, me, :, pl.ds(j * LANES, LANES)] = jnp.sum(acc[j], axis=0, keepdims=True)

    def sum_copy(a, d):
        peer = lax.rem(me + d, F)
        return pltpu.make_async_remote_copy(
            src_ref=sums.at[a, me], dst_ref=sums.at[a, me],
            send_sem=sum_send.at[a, d], recv_sem=sum_recv.at[a, me],
            device_id=(peer, col), device_id_type=MESH)

    def sum_arrival(a, f):
        return pltpu.make_async_remote_copy(
            src_ref=sums.at[a, f], dst_ref=sums.at[a, f],
            send_sem=sum_send.at[a, 0], recv_sem=sum_recv.at[a, f],
            device_id=(f, col), device_id_type=MESH)

    def norm_copy1(d):
        return pltpu.make_async_remote_copy(
            src_ref=norm_out.at[me, col], dst_ref=norm_out.at[me, col],
            send_sem=norm_send1.at[d], recv_sem=norm_recv1.at[col],
            device_id=(me, lax.rem(col + d, C)), device_id_type=MESH)

    def norm_copy2(d):
        return pltpu.make_async_remote_copy(
            src_ref=norm_out.at[me], dst_ref=norm_out.at[me],
            send_sem=norm_send2.at[d], recv_sem=norm_recv2.at[me],
            device_id=(lax.rem(me + d, F), col), device_id_type=MESH)

    mix(0)
    pl.semaphore_wait(barrier, F - 1 + C - 1)
    for d in range(1, F):
        sum_copy(0, d).start()
    for d in range(1, C):
        norm_copy1(d).start()
    mix(1)
    for d in range(1, F):
        sum_copy(1, d).start()
    mix(2)
    for d in range(1, F):
        sum_copy(2, d).start()

    def piece(a, source, q):
        start = pl.multiple_of(source * rows + q * part, part)
        return outs[a].at[pl.ds(start, part), :]

    def send(a, source, q, target, sender, receiver):
        ref = piece(a, source, q)
        return pltpu.make_async_remote_copy(
            src_ref=ref, dst_ref=ref, send_sem=sender, recv_sem=receiver,
            device_id=(target, col), device_id_type=MESH)

    def up(a, s, q):
        n = s * K + a * CHUNKS + q
        return send(a, 2 * s + core, q, me + 2, up_send.at[n], line_recv.at[n])

    def down(a, s, q):
        n = s * K + a * CHUNKS + q
        return send(a, 2 * s + core, q, me - 2, down_send.at[n], line_recv.at[n])

    def pair(a, s, q):
        n = s * K + a * CHUNKS + q
        return send(a, 2 * s + core, q, 2 * z + 1 - core, pair_send.at[n], pair_recv.at[n])

    def pair_arrival(a, s, q):
        n = s * K + a * CHUNKS + q
        return send(a, 2 * s + 1 - core, q, 2 * z + 1 - core, pair_send.at[n], pair_recv.at[n])

    def start_own(a, q):
        @pl.when(z > 0)
        def _():
            down(a, z, q).start()

        @pl.when(z < Z - 1)
        def _():
            up(a, z, q).start()

        pair(a, z, q).start()

    waiting = None
    for a in range(3):
        for d in range(1, F):
            sum_arrival(a, lax.rem(me + d, F)).wait_recv()
        total = sums[a, 0]
        for f in range(1, F):
            total = total + sums[a, f]
        scale = jnp.sqrt(total)
        scale_out[a] = scale
        inverse = jnp.broadcast_to(1.0 / scale, (16, width))
        for q in range(CHUNKS):
            base = me * rows + q * part

            def body(i, carry, a=a, q=q, base=base, inverse=inverse):
                r = pl.ds(pl.multiple_of(q * part + i * 16, 16), 16)
                o = pl.ds(pl.multiple_of(base + i * 16, 16), 16)
                outs[a][o, :] = (held[2 * a, r, :] * inverse).astype(jnp.bfloat16)
                return carry

            lax.fori_loop(0, part // 16, body, 0, unroll=2)
            if waiting is not None:
                start_own(*waiting)
            waiting = (a, q)
    for d in range(1, C):
        other = lax.rem(col + d, C)
        pltpu.make_async_remote_copy(
            src_ref=norm_out.at[me, other], dst_ref=norm_out.at[me, other],
            send_sem=norm_send1.at[0], recv_sem=norm_recv1.at[other],
            device_id=(me, other), device_id_type=MESH).wait_recv()
    for d in range(1, F):
        norm_copy2(d).start()
    start_own(*waiting)

    def relay(t, carry):
        hop = t // CHUNKS // 3 + 1
        q = lax.rem(t, CHUNKS)
        kind = lax.rem(t // CHUNKS, 3)
        for a in range(3):
            @pl.when(jnp.logical_and(kind == a, z + hop < Z))
            def _(a=a):
                down(a, z + hop, q).wait_recv()

                @pl.when(z > 0)
                def _():
                    down(a, z + hop, q).start()

                pair(a, z + hop, q).start()

            @pl.when(jnp.logical_and(kind == a, z - hop >= 0))
            def _(a=a):
                up(a, z - hop, q).wait_recv()

                @pl.when(z < Z - 1)
                def _():
                    up(a, z - hop, q).start()

                pair(a, z - hop, q).start()

        return carry

    lax.fori_loop(0, (Z - 1) * K, relay, 0)

    for d in range(1, F):
        f = lax.rem(me + d, F)
        pltpu.make_async_remote_copy(
            src_ref=norm_out.at[f], dst_ref=norm_out.at[f],
            send_sem=norm_send2.at[0], recv_sem=norm_recv2.at[f],
            device_id=(f, col), device_id_type=MESH).wait_recv()
        norm_copy2(d).wait_send()
        for a in range(3):
            sum_copy(a, d).wait_send()
    for d in range(1, C):
        norm_copy1(d).wait_send()

    def drain(n, carry):
        s = n // CHUNKS
        q = lax.rem(n, CHUNKS)
        for a in range(3):
            @pl.when(jnp.logical_and(z > 0, s >= z))
            def _(a=a):
                down(a, s, q).wait_send()

            @pl.when(jnp.logical_and(z < Z - 1, s <= z))
            def _(a=a):
                up(a, s, q).wait_send()

            pair_arrival(a, s, q).wait_recv()
            pair(a, s, q).wait_send()
        return carry

    lax.fori_loop(0, Z * CHUNKS, drain, 0)


def store_kernel(pieces, *refs):
    gathered, scales, norm = refs[0:3], refs[3], refs[4]
    finals, scale_outs, norm_out = refs[5:8], refs[8:11], refs[11]
    flat, sem = refs[12:]
    rows, width = gathered[0].shape
    part = rows // pieces
    copies = []
    for a in range(3):
        for p in range(pieces):
            r = pl.ds(p * part, part)
            copies.append(pltpu.make_async_copy(
                gathered[a].at[r, :], finals[a].at[r, :], sem.at[a * pieces + p]))
    for copy in copies:
        copy.start()
    for a in range(3):
        for j in range(width // LANES):
            scale_outs[a][pl.ds(j, 1), :] = scales[a, :, pl.ds(j * LANES, LANES)]
    F, C = norm.shape[0], norm.shape[1]
    for f in range(F):
        for c in range(C):
            flat[pl.ds(f * C + c, 1), :] = norm[f, c]
    norm_out[...] = flat[...].astype(jnp.bfloat16)
    for copy in copies:
        copy.wait()


def per_device(F, C, one_query, other_query, one_key, other_key, one_value, other_value,
               mix_share, norm_train, norm_step):
    rows, width = one_query.shape
    count = norm_train.shape[0]
    Z = F // 2
    K = 3 * CHUNKS
    whole = (F * rows, width)
    any_spec = pl.BlockSpec(memory_space=pl.ANY)
    vmem = pl.BlockSpec(memory_space=pltpu.VMEM)
    dma = pltpu.SemaphoreType.DMA
    sent = 3 * rows * width * 2 * Z
    gathered = pl.pallas_call(
        functools.partial(gather_kernel, F, C),
        out_shape=[pltpu.VMEM(whole, jnp.bfloat16)] * 3 + [
            pltpu.VMEM((3, 1, width), jnp.float32),
            pltpu.VMEM((F, C, 1, count), jnp.float32),
        ],
        in_specs=[pl.BlockSpec(memory_space=pltpu.HBM)] * 6 + [vmem] * 3,
        out_specs=[vmem] * 5,
        scratch_shapes=[
            pltpu.VMEM((6, rows, width), jnp.float32),
            pltpu.VMEM((rows, LANES), jnp.float32),
            pltpu.VMEM((3, F, 1, width), jnp.float32),
            dma((6,)),
            dma((3, F)), dma((3, F)),
            dma((C,)), dma((C,)),
            dma((F,)), dma((F,)),
            dma((Z * K,)), dma((Z * K,)), dma((Z * K,)), dma((Z * K,)), dma((Z * K,)),
        ],
        compiler_params=pltpu.CompilerParams(
            collective_id=0, has_side_effects=True, vmem_limit_bytes=VLIM),
        cost_estimate=pl.CostEstimate(flops=0, bytes_accessed=sent, transcendentals=0),
    )(one_query, other_query, one_key, other_key, one_value, other_value,
      mix_share.reshape(rows // LANES, LANES), norm_train.reshape(1, count),
      norm_step.reshape(1, count))
    pieces = 4
    finals = pl.pallas_call(
        functools.partial(store_kernel, pieces),
        out_shape=[jax.ShapeDtypeStruct(whole, jnp.bfloat16)] * 3
        + [jax.ShapeDtypeStruct((width // LANES, LANES), jnp.float32)] * 3
        + [jax.ShapeDtypeStruct((F * C, count), jnp.bfloat16)],
        in_specs=[vmem] * 5,
        out_specs=[any_spec] * 3 + [vmem] * 4,
        scratch_shapes=[pltpu.VMEM((F * C, count), jnp.float32), dma((3 * pieces,))],
        compiler_params=pltpu.CompilerParams(vmem_limit_bytes=VLIM2),
    )(*gathered)
    return (*finals[:3], *(s.reshape(width) for s in finals[3:6]), finals[6].reshape(F * C * count))


VLIM = 36 * 1024 * 1024
VLIM2 = 2 * 1024 * 1024


def solution(mesh):
    F, C = mesh.shape["fsdp"], mesh.shape["cols"]
    block, fsdp, both = P("fsdp", "cols"), P("fsdp"), P(("fsdp", "cols"))
    return jax.shard_map(
        functools.partial(per_device, F, C), mesh=mesh,
        in_specs=(block,) * 6 + (fsdp, both, both),
        out_specs=(P(None, "cols"),) * 3 + (P("cols"),) * 3 + (P(),),
        check_vma=False)
```

```python
import functools

import jax
import jax.numpy as jnp
from jax import lax
from jax.experimental import pallas as pl
from jax.experimental.pallas import tpu as pltpu
from jax.sharding import PartitionSpec as P

MESH = pl.DeviceIdType.MESH
LANES = 128
PIECES = ((0, 0, 1), (0, 1, 1), (0, 2, 6), (1, 0, 8), (2, 0, 6), (2, 6, 2))
LOADS = 4


def gather_kernel(F, C, *refs):
    ins, mix_ref, train_ref, step_ref = refs[0:6], refs[6], refs[7], refs[8]
    outs, scale_out, norm_out = refs[9:12], refs[12], refs[13]
    (held, mixb, sums, in_sem, sum_send, sum_recv, norm_send1, norm_recv1,
     norm_send2, norm_recv2, up_send, down_send, pair_send, line_recv, pair_recv,
     early, early_send, early_recv) = refs[14:]
    rows, width = ins[0].shape
    Z = F // 2
    me = lax.axis_index("fsdp")
    col = lax.axis_index("cols")
    z = me // 2
    core = lax.rem(me, 2)
    eighth = rows // 8
    K = len(PIECES)

    def at(f):
        return {"fsdp": f}

    load_rows = rows // LOADS

    def load(i, p):
        r = pl.ds(p * load_rows, load_rows)
        return pltpu.make_async_copy(ins[i].at[r, :], held.at[i, r, :], in_sem.at[i, p])

    for p in range(LOADS):
        load(0, p).start()
        load(1, p).start()

    barrier = pltpu.get_barrier_semaphore()
    for d in range(1, F):
        pl.semaphore_signal(barrier, inc=1, device_id=(lax.rem(me + d, F), col), device_id_type=MESH)
    for d in range(1, C):
        pl.semaphore_signal(barrier, inc=1, device_id=(me, lax.rem(col + d, C)), device_id_type=MESH)

    for g in range(rows // LANES):
        row = mix_ref[pl.ds(g, 1), :]
        mixb[pl.ds(g * LANES, LANES), :] = jnp.broadcast_to(row, (LANES, LANES)).T
    norm_out[me, col] = train_ref[...] + step_ref[...]

    def mix(a):
        def body(i, acc):
            r = pl.ds(pl.multiple_of(i * 8, 8), 8)
            m = mixb[r, :]
            n = 1.0 - m
            new = []
            for j in range(width // LANES):
                c = pl.ds(j * LANES, LANES)
                v = m * held[2 * a, r, c] + n * held[2 * a + 1, r, c]
                held[2 * a, r, c] = v
                new.append(acc[j] + v * v)
            return tuple(new)

        zero = jnp.zeros((8, LANES), jnp.float32)
        acc = (zero,) * (width // LANES)
        for p in range(LOADS):
            load(2 * a, p).wait()
            load(2 * a + 1, p).wait()
            acc = lax.fori_loop(p * load_rows // 8, (p + 1) * load_rows // 8, body, acc, unroll=2)
            if a == 0 and p == LOADS - 2:
                for i in range(2, 6):
                    for later in range(LOADS):
                        load(i, later).start()
        for j in range(width // LANES):
            sums[a, me, :, pl.ds(j * LANES, LANES)] = jnp.sum(acc[j], axis=0, keepdims=True)

    def sum_copy(a, d):
        peer = lax.rem(me + d, F)
        return pltpu.make_async_remote_copy(
            src_ref=sums.at[a, me], dst_ref=sums.at[a, me],
            send_sem=sum_send.at[a, d], recv_sem=sum_recv.at[a, me],
            device_id=(peer, col), device_id_type=MESH)

    def sum_arrival(a, f):
        return pltpu.make_async_remote_copy(
            src_ref=sums.at[a, f], dst_ref=sums.at[a, f],
            send_sem=sum_send.at[a, 0], recv_sem=sum_recv.at[a, f],
            device_id=(f, col), device_id_type=MESH)

    def norm_copy1(d):
        return pltpu.make_async_remote_copy(
            src_ref=norm_out.at[me, col], dst_ref=norm_out.at[me, col],
            send_sem=norm_send1.at[d], recv_sem=norm_recv1.at[col],
            device_id=(me, lax.rem(col + d, C)), device_id_type=MESH)

    def norm_copy2(d):
        return pltpu.make_async_remote_copy(
            src_ref=norm_out.at[me], dst_ref=norm_out.at[me],
            send_sem=norm_send2.at[d], recv_sem=norm_recv2.at[me],
            device_id=(lax.rem(me + d, F), col), device_id_type=MESH)

    mix(0)
    pl.semaphore_wait(barrier, F - 1 + C - 1)
    for d in range(1, F):
        sum_copy(0, d).start()
    early_rows = pl.ds(0, eighth)
    early_down = pltpu.make_async_remote_copy(
        src_ref=held.at[0, early_rows, :], dst_ref=early, send_sem=early_send.at[0],
        recv_sem=early_recv, device_id=(me - 2, col), device_id_type=MESH)
    early_up = pltpu.make_async_remote_copy(
        src_ref=held.at[0, early_rows, :], dst_ref=early, send_sem=early_send.at[1],
        recv_sem=early_recv, device_id=(me + 2, col), device_id_type=MESH)

    @pl.when(z == 1)
    def _():
        early_down.start()

    @pl.when(z == Z - 2)
    def _():
        early_up.start()

    for d in range(1, C):
        norm_copy1(d).start()
    mix(1)
    for d in range(1, F):
        sum_copy(1, d).start()
    mix(2)
    for d in range(1, F):
        sum_copy(2, d).start()

    def send(k, source, target, sender, receiver):
        a, first, count = PIECES[k]
        start = pl.multiple_of(source * rows + first * eighth, eighth)
        ref = outs[a].at[pl.ds(start, count * eighth), :]
        return pltpu.make_async_remote_copy(
            src_ref=ref, dst_ref=ref, send_sem=sender, recv_sem=receiver,
            device_id=(target, col), device_id_type=MESH)

    def up(k, s):
        n = s * K + k
        return send(k, 2 * s + core, me + 2, up_send.at[n], line_recv.at[n])

    def down(k, s):
        n = s * K + k
        return send(k, 2 * s + core, me - 2, down_send.at[n], line_recv.at[n])

    def pair(k, s):
        n = s * K + k
        return send(k, 2 * s + core, 2 * z + 1 - core, pair_send.at[n], pair_recv.at[n])

    def pair_arrival(k, s):
        n = s * K + k
        return send(k, 2 * s + 1 - core, 2 * z + 1 - core, pair_send.at[n], pair_recv.at[n])

    def goes_down(k, s):
        return jnp.logical_and(z > 0, jnp.logical_or(z != 1, s != z)) if k == 0 else z > 0

    def goes_up(k, s):
        return jnp.logical_and(z < Z - 1, jnp.logical_or(z != Z - 2, s != z)) if k == 0 else z < Z - 1

    def start_own(k):
        @pl.when(goes_down(k, z))
        def _():
            down(k, z).start()

        @pl.when(goes_up(k, z))
        def _():
            up(k, z).start()

        pair(k, z).start()

    def normalize(a, source, target, count, inverse):
        def body(i, carry):
            r = pl.ds(pl.multiple_of(i * 16, 16), 16)
            o = pl.ds(pl.multiple_of(target + i * 16, 16), 16)
            outs[a][o, :] = (source[r, :] * inverse).astype(jnp.bfloat16)
            return carry

        lax.fori_loop(0, count // 16, body, 0, unroll=2)

    inverses = []
    for k, (a, first, count) in enumerate(PIECES):
        if len(inverses) == a:
            for d in range(1, F):
                sum_arrival(a, lax.rem(me + d, F)).wait_recv()
            total = sums[a, 0]
            for f in range(1, F):
                total = total + sums[a, f]
            scale = jnp.sqrt(total)
            scale_out[a] = scale
            inverses.append(1.0 / scale)
        inverse = jnp.broadcast_to(inverses[a], (16, width))
        size = count * eighth
        normalize(a, held.at[2 * a, pl.ds(first * eighth, size), :],
                  me * rows + first * eighth, size, inverse)
        if k > 0:
            start_own(k - 1)
    for d in range(1, C):
        other = lax.rem(col + d, C)
        pltpu.make_async_remote_copy(
            src_ref=norm_out.at[me, other], dst_ref=norm_out.at[me, other],
            send_sem=norm_send1.at[0], recv_sem=norm_recv1.at[other],
            device_id=(me, other), device_id_type=MESH).wait_recv()
    for d in range(1, F):
        norm_copy2(d).start()
    start_own(K - 1)

    def take_early(owner):
        early_down.wait_recv()
        inverse = jnp.broadcast_to(1.0 / scale_out[0], (16, width))
        normalize(0, early, (2 * owner + core) * rows, eighth, inverse)

    def relay(hop, carry):
        for k in range(K):
            @pl.when(z + hop < Z)
            def _(k=k):
                if k == 0:
                    is_early = jnp.logical_and(z == 0, hop == 1)

                    @pl.when(is_early)
                    def _():
                        take_early(1)

                    @pl.when(jnp.logical_not(is_early))
                    def _():
                        down(k, z + hop).wait_recv()
                else:
                    down(k, z + hop).wait_recv()

                @pl.when(z > 0)
                def _():
                    down(k, z + hop).start()

                pair(k, z + hop).start()

            @pl.when(z - hop >= 0)
            def _(k=k):
                if k == 0:
                    is_early = jnp.logical_and(z == Z - 1, hop == 1)

                    @pl.when(is_early)
                    def _():
                        take_early(Z - 2)

                    @pl.when(jnp.logical_not(is_early))
                    def _():
                        up(k, z - hop).wait_recv()
                else:
                    up(k, z - hop).wait_recv()

                @pl.when(z < Z - 1)
                def _():
                    up(k, z - hop).start()

                pair(k, z - hop).start()

        return carry

    lax.fori_loop(1, Z, relay, 0)

    @pl.when(z == 1)
    def _():
        early_down.wait_send()

    @pl.when(z == Z - 2)
    def _():
        early_up.wait_send()

    for d in range(1, F):
        f = lax.rem(me + d, F)
        pltpu.make_async_remote_copy(
            src_ref=norm_out.at[f], dst_ref=norm_out.at[f],
            send_sem=norm_send2.at[0], recv_sem=norm_recv2.at[f],
            device_id=(f, col), device_id_type=MESH).wait_recv()
        norm_copy2(d).wait_send()
        for a in range(3):
            sum_copy(a, d).wait_send()
    for d in range(1, C):
        norm_copy1(d).wait_send()

    def drain(s, carry):
        for k in range(K):
            @pl.when(jnp.logical_and(goes_down(k, s), s >= z))
            def _(k=k):
                down(k, s).wait_send()

            @pl.when(jnp.logical_and(goes_up(k, s), s <= z))
            def _(k=k):
                up(k, s).wait_send()

            pair_arrival(k, s).wait_recv()
            pair(k, s).wait_send()
        return carry

    lax.fori_loop(0, Z, drain, 0)


def store_kernel(pieces, *refs):
    gathered, scales, norm = refs[0:3], refs[3], refs[4]
    finals, scale_outs, norm_out = refs[5:8], refs[8:11], refs[11]
    flat, flat_norm, flat_scales, sem, small_sem = refs[12:]
    rows, width = gathered[0].shape
    part = rows // pieces
    copies = []
    for a in range(3):
        for p in range(pieces):
            r = pl.ds(p * part, part)
            copies.append(pltpu.make_async_copy(
                gathered[a].at[r, :], finals[a].at[r, :], sem.at[a * pieces + p]))
    for copy in copies:
        copy.start()
    for a in range(3):
        for j in range(width // LANES):
            flat_scales[a, pl.ds(j, 1), :] = scales[a, :, pl.ds(j * LANES, LANES)]
    F, C = norm.shape[0], norm.shape[1]
    for f in range(F):
        for c in range(C):
            flat[pl.ds(f * C + c, 1), :] = norm[f, c]
    flat_norm[...] = flat[...].astype(jnp.bfloat16)
    small = [pltpu.make_async_copy(flat_scales.at[a], scale_outs[a], small_sem.at[a]) for a in range(3)]
    small.append(pltpu.make_async_copy(flat_norm, norm_out, small_sem.at[3]))
    for copy in small:
        copy.start()
    copies += small
    for copy in copies:
        copy.wait()


def per_device(F, C, one_query, other_query, one_key, other_key, one_value, other_value,
               mix_share, norm_train, norm_step):
    rows, width = one_query.shape
    count = norm_train.shape[0]
    Z = F // 2
    K = len(PIECES)
    whole = (F * rows, width)
    any_spec = pl.BlockSpec(memory_space=pl.ANY)
    vmem = pl.BlockSpec(memory_space=pltpu.VMEM)
    dma = pltpu.SemaphoreType.DMA
    sent = 3 * rows * width * 2 * Z
    gathered = pl.pallas_call(
        functools.partial(gather_kernel, F, C),
        out_shape=[pltpu.VMEM(whole, jnp.bfloat16)] * 3 + [
            pltpu.VMEM((3, 1, width), jnp.float32),
            pltpu.VMEM((F, C, 1, count), jnp.float32),
        ],
        in_specs=[pl.BlockSpec(memory_space=pltpu.HBM)] * 6 + [vmem] * 3,
        out_specs=[vmem] * 5,
        scratch_shapes=[
            pltpu.VMEM((6, rows, width), jnp.float32),
            pltpu.VMEM((rows, LANES), jnp.float32),
            pltpu.VMEM((3, F, 1, width), jnp.float32),
            dma((6, LOADS)),
            dma((3, F)), dma((3, F)),
            dma((C,)), dma((C,)),
            dma((F,)), dma((F,)),
            dma((Z * K,)), dma((Z * K,)), dma((Z * K,)), dma((Z * K,)), dma((Z * K,)),
            pltpu.VMEM((rows // 8, width), jnp.float32), dma((2,)), dma,
        ],
        compiler_params=pltpu.CompilerParams(
            collective_id=0, has_side_effects=True, vmem_limit_bytes=VLIM),
        cost_estimate=pl.CostEstimate(flops=0, bytes_accessed=sent, transcendentals=0),
    )(one_query, other_query, one_key, other_key, one_value, other_value,
      mix_share.reshape(rows // LANES, LANES), norm_train.reshape(1, count),
      norm_step.reshape(1, count))
    pieces = 4
    finals = pl.pallas_call(
        functools.partial(store_kernel, pieces),
        out_shape=[jax.ShapeDtypeStruct(whole, jnp.bfloat16)] * 3
        + [jax.ShapeDtypeStruct((width // LANES, LANES), jnp.float32)] * 3
        + [jax.ShapeDtypeStruct((F * C, count), jnp.bfloat16)],
        in_specs=[vmem] * 5,
        out_specs=[any_spec] * 7,
        scratch_shapes=[
            pltpu.VMEM((F * C, count), jnp.float32), pltpu.VMEM((F * C, count), jnp.bfloat16),
            pltpu.VMEM((3, width // LANES, LANES), jnp.float32), dma((3 * pieces,)), dma((4,)),
        ],
        compiler_params=pltpu.CompilerParams(vmem_limit_bytes=VLIM2),
    )(*gathered)
    return (*finals[:3], *(s.reshape(width) for s in finals[3:6]), finals[6].reshape(F * C * count))


VLIM = 36 * 1024 * 1024
VLIM2 = 2 * 1024 * 1024


def solution(mesh):
    F, C = mesh.shape["fsdp"], mesh.shape["cols"]
    block, fsdp, both = P("fsdp", "cols"), P("fsdp"), P(("fsdp", "cols"))
    return jax.shard_map(
        functools.partial(per_device, F, C), mesh=mesh,
        in_specs=(block,) * 6 + (fsdp, both, both),
        out_specs=(P(None, "cols"),) * 3 + (P("cols"),) * 3 + (P(),),
        check_vma=False)
```
